32 devices in a mesh: ctx: 16 (over z, y, x), tp: 2 (over core).
Axes of the slice: x: 2, y: 2, z: 4, core: 2. Of those that a mesh axis runs over, the one named last changes fastest.
Arguments:
- rotated_asking_vectors: bfloat16 [2, 512, 64, 128], P(None, ('ctx', 'tp')), may hold values from -6 to 6
- rotated_match_vectors: bfloat16 [2, 512, 8, 128], P(None, ('ctx', 'tp')), may hold values from -6 to 6
- content_vectors: bfloat16 [2, 512, 8, 128], P(None, ('ctx', 'tp')), may hold values from -6 to 6
- result_cotangent: bfloat16 [2, 512, 64, 128], P(None, ('ctx', 'tp')), may hold values from -6 to 6
Outputs:
- attended: bfloat16 [2, 512, 64, 128], P(None, ('ctx', 'tp'))
- grad_query: bfloat16 [2, 512, 64, 128], P(None, ('ctx', 'tp'))
- grad_key: bfloat16 [2, 512, 8, 128], P(None, ('ctx', 'tp'))
- grad_value: bfloat16 [2, 512, 8, 128], P(None, ('ctx', 'tp'))
The draws below stay inside these ranges and needn't reach their ends.
All inputs are finite; a program needn't handle non-finite values.
Results may differ from the reference program's by a relative error of at most 0.002.
Values may be sent and summed in bfloat16 or wider, within the bound.
A program may use at most 64 MiB of HBM per device.

```python
import jax
import jax.numpy as jnp
from jax import lax

ASKING_HEAD_COUNT = 64
SHARED_HEAD_COUNT = 8
HEAD_WIDTH = 128
DEPTH_COUNT = 2
WINDOW_LENGTH = 512
QUERIES_PER_SHARED = 8


def level_of(key, extent, cuts, least, top_value):
    loudness, own = 1.0, jax.random.fold_in(key, 6)
    for position, parts in cuts:
        steps = jnp.exp(jax.random.uniform(jax.random.fold_in(own, position), (parts,), jnp.float32, least / len(cuts), top_value / len(cuts)))
        loudness = loudness * jnp.repeat(steps, extent[position] // parts).reshape([-1 if axis == position else 1 for axis in range(len(extent))])
    return loudness


def noise(rng, shape, spread, reach, pieces=(), kind=jnp.bfloat16):
    result = spread * jax.random.normal(rng, shape, jnp.float32)
    if pieces:
        result = result * level_of(rng, shape, pieces, -0.22, 0.18)
    return jnp.clip(result, -reach, reach).astype(kind)


def setup_inputs(seed: int = 0) -> dict:
    key_list = jax.random.split(jax.random.key(seed), 5)
    return {
        "rotated_asking_vectors": noise(key_list[0], (DEPTH_COUNT, WINDOW_LENGTH, ASKING_HEAD_COUNT, HEAD_WIDTH), 1.0, 6.0, ((1, 32),)),
        "rotated_match_vectors": noise(key_list[1], (DEPTH_COUNT, WINDOW_LENGTH, SHARED_HEAD_COUNT, HEAD_WIDTH), 1.0, 6.0, ((1, 32),)),
        "content_vectors": noise(key_list[2], (DEPTH_COUNT, WINDOW_LENGTH, SHARED_HEAD_COUNT, HEAD_WIDTH), 1.0, 6.0, ((1, 32),)),
        "result_cotangent": noise(key_list[3], (DEPTH_COUNT, WINDOW_LENGTH, ASKING_HEAD_COUNT, HEAD_WIDTH), 1.0, 6.0, ((1, 32),)),
    }


def head_group(operands):
    query_group, key_group, value_group, grad_group = operands
    softmax_scale = HEAD_WIDTH ** -0.5
    places = jnp.arange(WINDOW_LENGTH, dtype=jnp.int32)
    causal_mask = places[None, :] <= places[:, None]
    scores = jnp.einsum("gid,jd->gij", query_group, key_group, precision=lax.Precision.HIGHEST) * softmax_scale
    scores = jnp.where(causal_mask[None], scores, -jnp.inf)
    highest = jnp.max(scores, axis=-1, keepdims=True)
    log_norm = highest + jnp.log(jnp.sum(jnp.exp(scores - highest), axis=-1, keepdims=True))
    probabilities = jnp.exp(scores - log_norm)
    attended = jnp.einsum("gij,jd->gid", probabilities, value_group, precision=lax.Precision.HIGHEST).astype(jnp.bfloat16)
    saved_out = lax.optimization_barrier(attended).astype(jnp.float32)
    row_delta = jnp.sum(grad_group * saved_out, axis=-1, keepdims=True)
    prob_grad = jnp.einsum("gid,jd->gij", grad_group, value_group, precision=lax.Precision.HIGHEST)
    dscore = probabilities * (prob_grad - row_delta)
    query_grad = softmax_scale * jnp.einsum("gij,jd->gid", dscore, key_group, precision=lax.Precision.HIGHEST)
    key_grad = softmax_scale * jnp.einsum("gij,gid->jd", dscore, query_group, precision=lax.Precision.HIGHEST)
    value_grad = jnp.einsum("gij,gid->jd", probabilities, grad_group, precision=lax.Precision.HIGHEST)
    return attended, query_grad.astype(jnp.bfloat16), key_grad.astype(jnp.bfloat16), value_grad.astype(jnp.bfloat16)


def reference(rotated_asking_vectors, rotated_match_vectors, content_vectors, result_cotangent):
    outputs = ([], [], [], [])
    for depth_position in range(DEPTH_COUNT):
        expanded_asking_vectors = rotated_asking_vectors[depth_position].astype(jnp.float32).reshape(WINDOW_LENGTH, SHARED_HEAD_COUNT, QUERIES_PER_SHARED, HEAD_WIDTH).transpose(1, 2, 0, 3)
        expanded_cotangent = result_cotangent[depth_position].astype(jnp.float32).reshape(WINDOW_LENGTH, SHARED_HEAD_COUNT, QUERIES_PER_SHARED, HEAD_WIDTH).transpose(1, 2, 0, 3)
        key_wide = rotated_match_vectors[depth_position].astype(jnp.float32).transpose(1, 0, 2)
        value_wide = content_vectors[depth_position].astype(jnp.float32).transpose(1, 0, 2)
        attended, query_grad, key_grad, value_grad = lax.map(head_group, (expanded_asking_vectors, key_wide, value_wide, expanded_cotangent))
        outputs[0].append(attended.transpose(2, 0, 1, 3).reshape(WINDOW_LENGTH, ASKING_HEAD_COUNT, HEAD_WIDTH))
        outputs[1].append(query_grad.transpose(2, 0, 1, 3).reshape(WINDOW_LENGTH, ASKING_HEAD_COUNT, HEAD_WIDTH))
        outputs[2].append(key_grad.transpose(1, 0, 2))
        outputs[3].append(value_grad.transpose(1, 0, 2))
    return (jnp.stack(outputs[0]), jnp.stack(outputs[1]), jnp.stack(outputs[2]), jnp.stack(outputs[3]))
```

```python
from functools import partial

import jax
import jax.numpy as jnp
from jax import lax
from jax.experimental import pallas as pl
from jax.experimental.pallas import tpu as pltpu
from jax.sharding import PartitionSpec as P

MESH = pl.DeviceIdType.MESH
masked_score = -1e30
F32, BF16 = jnp.float32, jnp.bfloat16


def dot(a, b, dims=((1,), (0,))):
    return lax.dot_general(a, b, (dims, ((), ())), preferred_element_type=F32)


def halves(x):
    high = x.astype(BF16)
    return high, (x - high.astype(F32)).astype(BF16)


def kernel(
    sizes,
    qg_ref,
    kv_ref,
    og_ref,
    okv_ref,
    qgb,
    kvb,
    out_qg,
    acc,
    recv,
    out_kv,
    wide,
    turned,
    kv_s,
    kv_r,
    qg_s,
    qg_r,
    z_s,
    z_r,
    p_s,
    p_r,
    o_s,
    o_r,
    f_s,
    f_r,
    local,
):
    layers, inner, outer, tp_n, t, heads, width = sizes
    G = inner * tp_n
    B = G * t
    T = outer * B
    rows = t * heads
    scale = width**-0.5
    ctx, tp = lax.axis_index("ctx"), lax.axis_index("tp")
    z = ctx // inner
    me = (ctx % inner) * tp_n + tp

    def in_plane(peer):
        return {"ctx": z * inner + peer // tp_n, "tp": peer % tp_n}

    def in_column(o):
        return {"ctx": o * inner + ctx % inner, "tp": tp}

    def kv_copy(l, to, slot):
        return pltpu.make_async_remote_copy(
            kv_ref.at[to, l], kvb.at[l, z, slot], kv_s.at[l, to], kv_r.at[l, slot], in_plane(to), MESH
        )

    def qg_copy(l, to, slot):
        return pltpu.make_async_remote_copy(
            qg_ref.at[to, l], qgb.at[l, slot], qg_s.at[l, to], qg_r.at[l, slot], in_plane(to), MESH
        )

    def z_copy(l, to, slot):
        return pltpu.make_async_remote_copy(
            kvb.at[l, slot], kvb.at[l, slot], z_s.at[l, to], z_r.at[l, slot], in_column(to), MESH
        )

    def p_copy(l, to, slot):
        return pltpu.make_async_remote_copy(
            acc.at[l, to], recv.at[l, slot], p_s.at[l, to], p_r.at[l, slot], in_column(to), MESH
        )

    def o_copy(l, to, slot):
        return pltpu.make_async_remote_copy(
            out_qg.at[l, to], og_ref.at[slot, l], o_s.at[l, to], o_r.at[l, slot], in_plane(to), MESH
        )

    def f_copy(l, to, slot):
        return pltpu.make_async_remote_copy(
            out_kv.at[l, to], okv_ref.at[slot, l], f_s.at[l, to], f_r.at[l, slot], in_plane(to), MESH
        )

    def each_peer(fn):
        for d in range(1, G):
            fn(lax.rem(me + d, G))

    barrier = pltpu.get_barrier_semaphore()
    each_peer(lambda p: pl.semaphore_signal(barrier, 1, device_id=in_plane(p), device_id_type=MESH))

    @pl.loop(1, outer)
    def _(d):
        pl.semaphore_signal(
            barrier, 1, device_id=in_column(lax.rem(z + d, outer)), device_id_type=MESH
        )

    pl.semaphore_wait(barrier, G - 1 + outer - 1)

    for l in range(layers):
        each_peer(lambda p: kv_copy(l, p, me).start())
    for l in range(layers):
        each_peer(lambda p: qg_copy(l, p, me).start())
    own = []
    for l in range(layers):
        own.append(pltpu.make_async_copy(kv_ref.at[me, l], kvb.at[l, z, me], local.at[l, 0]))
        own.append(pltpu.make_async_copy(qg_ref.at[me, l], qgb.at[l, me], local.at[l, 1]))
    for copy in own:
        copy.start()
    for l in range(layers):

        @pl.loop(z + 1, outer)
        def _(o):
            kvb[l, o] = jnp.zeros(kvb.shape[2:], BF16)

    for copy in own:
        copy.wait()
    for l in range(layers):
        each_peer(lambda p: kv_copy(l, me, p).wait_recv())

        @pl.loop(z + 1, outer)
        def _(o):
            z_copy(l, o, z).start()

    n = max(1, min(G, 256 // rows))
    c = n * rows

    def whole(l, kind):
        if t % 16 == 0:
            return kvb[l, :, :, kind].reshape(T, width)
        return wide[kind].reshape(T, width).astype(BF16)

    for l in range(layers):
        each_peer(lambda p: qg_copy(l, me, p).wait_recv())

        @pl.loop(0, z)
        def _(o):
            z_copy(l, me * 0 + o, o).wait_recv()

        if t % 16:

            @pl.loop(0, outer)
            def _(o):
                for p in range(G):
                    for kind in range(2):
                        wide[kind, o, p * t : (p + 1) * t, :] = kvb[l, o, p, kind].astype(F32)

        for kind in range(2):
            turned[kind] = whole(l, kind).astype(F32).T.astype(BF16)
        acc[l] = jnp.zeros(acc.shape[1:], F32)

        @pl.loop(0, G // n)
        def _(ci):
            K, V = whole(l, 0), whole(l, 1)
            span = pl.ds(ci * n, n)
            Q = qgb[l, span, 0].reshape(c, width)
            dO = qgb[l, span, 1].reshape(c, width)
            token = z * B + (ci * c + lax.broadcasted_iota(jnp.int32, (1, c), 1)) // heads
            allowed = lax.broadcasted_iota(jnp.int32, (T, c), 0) <= token
            scores = jnp.where(allowed, dot(K, Q, ((1,), (1,))) * scale, masked_score)
            e = jnp.exp(scores - jnp.max(scores, axis=0, keepdims=True))
            prob = e * (1.0 / jnp.sum(e, axis=0, keepdims=True))
            ph, pe = halves(prob)
            att = (dot(turned[1], ph) + dot(turned[1], pe)).T.astype(BF16)
            out_qg[l, span, 0] = att.reshape(n, rows, width)
            delta = jnp.sum((att.astype(F32) * dO.astype(F32)).T, axis=0, keepdims=True)
            dscore = prob * (dot(V, dO, ((1,), (1,))) - delta)
            dh, de = halves(dscore)
            dq = ((dot(turned[0], dh) + dot(turned[0], de)) * scale).T.astype(BF16)
            out_qg[l, span, 1] = dq.reshape(n, rows, width)
            acc[l, :, 0] += (dot(dh, Q) + dot(de, Q)).reshape(outer, B, width)
            acc[l, :, 1] += (dot(ph, dO) + dot(pe, dO)).reshape(outer, B, width)
            for i in range(n):
                peer = ci * n + i

                @pl.when(peer != me)
                def _():
                    o_copy(l, peer, me).start()

        @pl.loop(0, z)
        def _(o):
            p_copy(l, o, z).start()

        pltpu.make_async_copy(out_qg.at[l, me], og_ref.at[me, l], local.at[l, 2]).start()

    for l in range(layers):

        @pl.loop(z + 1, outer)
        def _(o):
            p_copy(l, z, o).wait_recv()
            acc[l, z] += recv[l, o]

        for kind in range(2):
            factor = scale if kind == 0 else 1.0
            for p in range(G):
                out_kv[l, p, kind] = (acc[l, z, kind, p * t : (p + 1) * t, :] * factor).astype(BF16)
        each_peer(lambda p: f_copy(l, p, me).start())
        pltpu.make_async_copy(out_kv.at[l, me], okv_ref.at[me, l], local.at[l, 3]).start()

    for l in range(layers):
        pltpu.make_async_copy(out_qg.at[l, me], og_ref.at[me, l], local.at[l, 2]).wait()
        pltpu.make_async_copy(out_kv.at[l, me], okv_ref.at[me, l], local.at[l, 3]).wait()

        def finish(p):
            kv_copy(l, p, me).wait_send()
            qg_copy(l, p, me).wait_send()
            o_copy(l, p, me).wait_send()
            f_copy(l, p, me).wait_send()
            o_copy(l, me, p).wait_recv()
            f_copy(l, me, p).wait_recv()

        each_peer(finish)

        @pl.loop(z + 1, outer)
        def _(o):
            z_copy(l, o, z).wait_send()

        @pl.loop(0, z)
        def _(o):
            p_copy(l, o, z).wait_send()


def on_device(q, k, v, g):
    layers, t, head_count, width = q.shape
    kv_heads = k.shape[2]
    heads = head_count // kv_heads
    ctx_n, tp_n = lax.axis_size("ctx"), lax.axis_size("tp")
    inner = kv_heads // tp_n
    outer = ctx_n // inner
    G, B, rows = kv_heads, kv_heads * t, t * heads

    def pack(a, b):
        both = jnp.stack([a, b]).reshape(2, layers, t, kv_heads, -1, width)
        return both.transpose(3, 1, 0, 2, 4, 5).reshape(kv_heads, layers, 2, -1, width)

    def unpack(both):
        both = both.reshape(kv_heads, layers, 2, t, -1, width).transpose(2, 1, 3, 0, 4, 5)
        both = both.reshape(2, layers, t, -1, width)
        return both[0], both[1]

    vmem = pl.BlockSpec(memory_space=pltpu.VMEM)
    sem = pltpu.SemaphoreType.DMA
    plane, column = sem((layers, G)), sem((layers, outer))
    qg_shape = (kv_heads, layers, 2, rows, width)
    kv_shape = (kv_heads, layers, 2, t, width)
    og, okv = pl.pallas_call(
        partial(kernel, (layers, inner, outer, tp_n, t, heads, width)),
        out_shape=(jax.ShapeDtypeStruct(qg_shape, BF16), jax.ShapeDtypeStruct(kv_shape, BF16)),
        in_specs=[vmem, vmem],
        out_specs=(vmem, vmem),
        scratch_shapes=[
            pltpu.VMEM((layers, G, 2, rows, width), BF16),
            pltpu.VMEM((layers, outer, G, 2, t, width), BF16),
            pltpu.VMEM((layers, G, 2, rows, width), BF16),
            pltpu.VMEM((layers, outer, 2, B, width), F32),
            pltpu.VMEM((layers, outer, 2, B, width), F32),
            pltpu.VMEM((layers, G, 2, t, width), BF16),
            pltpu.VMEM((2, outer, B, width) if t % 16 else (2, 1, 8, width), F32),
            pltpu.VMEM((2, width, outer * B), BF16),
            plane,
            plane,
            plane,
            plane,
            column,
            column,
            column,
            column,
            plane,
            plane,
            plane,
            plane,
            sem((layers, 4)),
        ],
        compiler_params=pltpu.CompilerParams(collective_id=0, has_side_effects=True),
    )(pack(q, g), pack(k, v))
    attended, grad_query = unpack(og)
    grad_key, grad_value = unpack(okv)
    return attended, grad_query, grad_key, grad_value


def solution(mesh):
    spec = P(None, ("ctx", "tp"), None, None)
    return jax.shard_map(
        on_device, mesh=mesh, in_specs=(spec,) * 4, out_specs=(spec,) * 4, check_vma=False
    )
```

```python
from functools import partial

import jax
import jax.numpy as jnp
from jax import lax
from jax.experimental import pallas as pl
from jax.experimental.pallas import tpu as pltpu
from jax.sharding import PartitionSpec as P

MESH = pl.DeviceIdType.MESH
masked_score = -1e30
F32, BF16 = jnp.float32, jnp.bfloat16


def dot(a, b, dims=((1,), (0,))):
    return lax.dot_general(a, b, (dims, ((), ())), preferred_element_type=F32)


def halves(x):
    high = x.astype(BF16)
    return high, (x - high.astype(F32)).astype(BF16)


def kernel(
    sizes,
    q_ref,
    g_ref,
    kv_ref,
    att_ref,
    dq_ref,
    okv_ref,
    qgb,
    kvb,
    out_qg,
    acc,
    recv,
    out_kv,
    wide,
    turned,
    kv_s,
    kv_r,
    qg_s,
    qg_r,
    z_s,
    z_r,
    p_s,
    p_r,
    o_s,
    o_r,
    f_s,
    f_r,
    local,
):
    layers, inner, outer, tp_n, t, heads, width = sizes
    G = inner * tp_n
    B = G * t
    T = outer * B
    rows = t * heads
    scale = width**-0.5
    ctx, tp = lax.axis_index("ctx"), lax.axis_index("tp")
    z = ctx // inner
    me = (ctx % inner) * tp_n + tp

    def in_plane(peer):
        return {"ctx": z * inner + peer // tp_n, "tp": peer % tp_n}

    def in_column(o):
        return {"ctx": o * inner + ctx % inner, "tp": tp}

    def kv_copy(l, to, slot):
        return pltpu.make_async_remote_copy(
            kv_ref.at[to, l], kvb.at[l, z, slot], kv_s.at[l, to], kv_r.at[l, slot], in_plane(to), MESH
        )

    def group(ref, l, peer):
        return ref.at[l, :, pl.ds(pl.multiple_of(peer * heads, heads), heads), :]

    def qg_copy(l, kind, to, slot):
        return pltpu.make_async_remote_copy(
            group((q_ref, g_ref)[kind], l, to),
            qgb.at[l, slot, kind],
            qg_s.at[l, kind, to],
            qg_r.at[l, kind, slot],
            in_plane(to),
            MESH,
        )

    def z_copy(l, to, slot):
        return pltpu.make_async_remote_copy(
            kvb.at[l, slot], kvb.at[l, slot], z_s.at[l, to], z_r.at[l, slot], in_column(to), MESH
        )

    def p_copy(l, to, slot):
        return pltpu.make_async_remote_copy(
            acc.at[l, to], recv.at[l, slot], p_s.at[l, to], p_r.at[l, slot], in_column(to), MESH
        )

    def o_copy(l, kind, to, slot):
        return pltpu.make_async_remote_copy(
            out_qg.at[l, to, kind],
            group((att_ref, dq_ref)[kind], l, slot),
            o_s.at[l, kind, to],
            o_r.at[l, kind, slot],
            in_plane(to),
            MESH,
        )

    def o_own(l, kind):
        return pltpu.make_async_copy(
            out_qg.at[l, me, kind], group((att_ref, dq_ref)[kind], l, me), local.at[l, 3 + kind]
        )

    def f_copy(l, to, slot):
        return pltpu.make_async_remote_copy(
            out_kv.at[l, to], okv_ref.at[slot, l], f_s.at[l, to], f_r.at[l, slot], in_plane(to), MESH
        )

    def each_peer(fn):
        for d in range(1, G):
            fn(lax.rem(me + d, G))

    barrier = pltpu.get_barrier_semaphore()
    each_peer(lambda p: pl.semaphore_signal(barrier, 1, device_id=in_plane(p), device_id_type=MESH))

    @pl.loop(1, outer)
    def _(d):
        pl.semaphore_signal(
            barrier, 1, device_id=in_column(lax.rem(z + d, outer)), device_id_type=MESH
        )

    pl.semaphore_wait(barrier, G - 1 + outer - 1)

    for l in range(layers):
        each_peer(lambda p: kv_copy(l, p, me).start())
    for l in range(layers):
        for kind in range(2):
            each_peer(lambda p: qg_copy(l, kind, p, me).start())
    own = []
    for l in range(layers):
        own.append(pltpu.make_async_copy(kv_ref.at[me, l], kvb.at[l, z, me], local.at[l, 0]))
        for kind, ref in enumerate((q_ref, g_ref)):
            own.append(
                pltpu.make_async_copy(group(ref, l, me), qgb.at[l, me, kind], local.at[l, 1 + kind])
            )
    for copy in own:
        copy.start()
    for l in range(layers):

        @pl.loop(z + 1, outer)
        def _(o):
            kvb[l, o] = jnp.zeros(kvb.shape[2:], BF16)

    for copy in own:
        copy.wait()
    for l in range(layers):
        each_peer(lambda p: kv_copy(l, me, p).wait_recv())

        @pl.loop(z + 1, outer)
        def _(o):
            z_copy(l, o, z).start()

    n = max(1, min(G, 256 // rows))
    c = n * rows

    def whole(l, kind):
        if t % 16 == 0:
            return kvb[l, :, :, kind].reshape(T, width)
        return wide[kind].reshape(T, width).astype(BF16)

    for l in range(layers):
        for kind in range(2):
            each_peer(lambda p: qg_copy(l, kind, me, p).wait_recv())

        @pl.loop(0, z)
        def _(o):
            z_copy(l, me * 0 + o, o).wait_recv()

        if t % 16:

            @pl.loop(0, outer)
            def _(o):
                for p in range(G):
                    for kind in range(2):
                        wide[kind, o, p * t : (p + 1) * t, :] = kvb[l, o, p, kind].astype(F32)

        for kind in range(2):
            turned[kind] = whole(l, kind).astype(F32).T.astype(BF16)
        acc[l] = jnp.zeros(acc.shape[1:], F32)

        @pl.loop(0, G // n)
        def _(ci):
            K, V = whole(l, 0), whole(l, 1)
            span = pl.ds(ci * n, n)
            Q = qgb[l, span, 0].reshape(c, width)
            dO = qgb[l, span, 1].reshape(c, width)
            token = z * B + (ci * c + lax.broadcasted_iota(jnp.int32, (1, c), 1)) // heads
            allowed = lax.broadcasted_iota(jnp.int32, (T, c), 0) <= token
            scores = jnp.where(allowed, dot(K, Q, ((1,), (1,))) * scale, masked_score)
            e = jnp.exp(scores - jnp.max(scores, axis=0, keepdims=True))
            prob = e * (1.0 / jnp.sum(e, axis=0, keepdims=True))
            ph, pe = halves(prob)
            att = (dot(turned[1], ph) + dot(turned[1], pe)).T.astype(BF16)
            out_qg[l, span, 0] = att.reshape(n, t, heads, width)
            delta = jnp.sum((att.astype(F32) * dO.astype(F32)).T, axis=0, keepdims=True)
            dscore = prob * (dot(V, dO, ((1,), (1,))) - delta)
            dh, de = halves(dscore)
            dq = ((dot(turned[0], dh) + dot(turned[0], de)) * scale).T.astype(BF16)
            out_qg[l, span, 1] = dq.reshape(n, t, heads, width)
            acc[l, :, 0] += (dot(dh, Q) + dot(de, Q)).reshape(outer, B, width)
            acc[l, :, 1] += (dot(ph, dO) + dot(pe, dO)).reshape(outer, B, width)
            for i in range(n):
                peer = ci * n + i

                @pl.when(peer != me)
                def _():
                    for kind in range(2):
                        o_copy(l, kind, peer, me).start()

        @pl.loop(0, z)
        def _(o):
            p_copy(l, o, z).start()

        for kind in range(2):
            o_own(l, kind).start()

    for l in range(layers):

        @pl.loop(z + 1, outer)
        def _(o):
            p_copy(l, z, o).wait_recv()
            acc[l, z] += recv[l, o]

        for kind in range(2):
            factor = scale if kind == 0 else 1.0
            for p in range(G):
                out_kv[l, p, kind] = (acc[l, z, kind, p * t : (p + 1) * t, :] * factor).astype(BF16)
        each_peer(lambda p: f_copy(l, p, me).start())
        pltpu.make_async_copy(out_kv.at[l, me], okv_ref.at[me, l], local.at[l, 5]).start()

    for l in range(layers):
        for kind in range(2):
            o_own(l, kind).wait()
        pltpu.make_async_copy(out_kv.at[l, me], okv_ref.at[me, l], local.at[l, 5]).wait()

        def finish(p):
            kv_copy(l, p, me).wait_send()
            for kind in range(2):
                qg_copy(l, kind, p, me).wait_send()
                o_copy(l, kind, p, me).wait_send()
                o_copy(l, kind, me, p).wait_recv()
            f_copy(l, p, me).wait_send()
            f_copy(l, me, p).wait_recv()

        each_peer(finish)

        @pl.loop(z + 1, outer)
        def _(o):
            z_copy(l, o, z).wait_send()

        @pl.loop(0, z)
        def _(o):
            p_copy(l, o, z).wait_send()


def on_device(q, k, v, g):
    layers, t, head_count, width = q.shape
    kv_heads = k.shape[2]
    heads = head_count // kv_heads
    ctx_n, tp_n = lax.axis_size("ctx"), lax.axis_size("tp")
    inner = kv_heads // tp_n
    outer = ctx_n // inner
    G, B = kv_heads, kv_heads * t

    def pack(a, b):
        both = jnp.stack([a, b]).reshape(2, layers, t, kv_heads, -1, width)
        return both.transpose(3, 1, 0, 2, 4, 5).reshape(kv_heads, layers, 2, -1, width)

    def unpack(both):
        both = both.reshape(kv_heads, layers, 2, t, -1, width).transpose(2, 1, 3, 0, 4, 5)
        both = both.reshape(2, layers, t, -1, width)
        return both[0], both[1]

    vmem = pl.BlockSpec(memory_space=pltpu.VMEM)
    sem = pltpu.SemaphoreType.DMA
    plane, column = sem((layers, G)), sem((layers, outer))
    pair = sem((layers, 2, G))
    whole_shape = jax.ShapeDtypeStruct(q.shape, BF16)
    kv_shape = (kv_heads, layers, 2, t, width)
    attended, grad_query, okv = pl.pallas_call(
        partial(kernel, (layers, inner, outer, tp_n, t, heads, width)),
        out_shape=(whole_shape, whole_shape, jax.ShapeDtypeStruct(kv_shape, BF16)),
        in_specs=[vmem, vmem, vmem],
        out_specs=(vmem, vmem, vmem),
        scratch_shapes=[
            pltpu.VMEM((layers, G, 2, t, heads, width), BF16),
            pltpu.VMEM((layers, outer, G, 2, t, width), BF16),
            pltpu.VMEM((layers, G, 2, t, heads, width), BF16),
            pltpu.VMEM((layers, outer, 2, B, width), F32),
            pltpu.VMEM((layers, outer, 2, B, width), F32),
            pltpu.VMEM((layers, G, 2, t, width), BF16),
            pltpu.VMEM((2, outer, B, width) if t % 16 else (2, 1, 8, width), F32),
            pltpu.VMEM((2, width, outer * B), BF16),
            plane,
            plane,
            pair,
            pair,
            column,
            column,
            column,
            column,
            pair,
            pair,
            plane,
            plane,
            sem((layers, 6)),
        ],
        compiler_params=pltpu.CompilerParams(collective_id=0, has_side_effects=True),
    )(q, g, pack(k, v))
    grad_key, grad_value = unpack(okv)
    return attended, grad_query, grad_key, grad_value


def solution(mesh):
    spec = P(None, ("ctx", "tp"), None, None)
    return jax.shard_map(
        on_device, mesh=mesh, in_specs=(spec,) * 4, out_specs=(spec,) * 4, check_vma=False
    )
```
